32 devices in a mesh: blk: 8 (over y, x, core), uly: 4 (over z).
Axes of the slice: x: 2, y: 2, z: 4, core: 2. Of those that a mesh axis runs over, the one named last changes fastest.
Arguments:
- self_query: bfloat16 [1280, 5120], P(('blk', 'uly')), may hold values from -8 to 8
- self_key: bfloat16 [1280, 5120], P(('blk', 'uly')), may hold values from -8 to 8
- self_value: bfloat16 [1280, 5120], P(('blk', 'uly')), may hold values from -6 to 6
- cross_query: bfloat16 [1280, 5120], P(('blk', 'uly')), may hold values from -8 to 8
- text_key: bfloat16 [512, 5120], P('blk', 'uly'), may hold values from -8 to 8
- text_value: bfloat16 [512, 5120], P('blk', 'uly'), may hold values from -6 to 6
- padded_count: int32 [1], replicated, may hold values from 0 to 320
Outputs:
- self_out: bfloat16 [1280, 5120], P(('blk', 'uly'))
- cross_out: bfloat16 [1280, 5120], P(('blk', 'uly'))
The draws below stay inside these ranges and needn't reach their ends.
All inputs are finite; a program needn't handle non-finite values.
Results may differ from the reference program's by a relative error of at most 0.0099.
Values may be sent and summed in bfloat16 or wider, within the bound.
No kernel may reach another device: no remote copies, remote signals or barrier semaphores. Data moves between devices by JAX's collectives and lax.ppermute only.
A program may use at most 128 MiB of HBM per device.

```python
import math
import jax
import jax.numpy as jnp
from jax import lax

HEADS = 40
HD = 128
TEXT = 512
TH = 4
TW = 10
ROW_TILES = 8
FRAMES = 1
GRID_H = 32
GRID_W = 40
TOKENS = 1280
N_ULY = 4


def draw_self_query(key, part):
    own_key = jax.random.fold_in(key, 1)
    values = 1.8 * jax.random.truncated_normal(own_key, -4.0, 4.0, (TOKENS, HEADS * HD), jnp.float32)
    return values.astype(jnp.bfloat16)


def draw_self_key(key, part):
    own_key = jax.random.fold_in(key, 2)
    values = 1.8 * jax.random.truncated_normal(own_key, -4.0, 4.0, (TOKENS, HEADS * HD), jnp.float32)
    return values.astype(jnp.bfloat16)


def draw_cross_query(key, part):
    own_key = jax.random.fold_in(key, 3)
    values = 1.6 * jax.random.truncated_normal(own_key, -4.0, 4.0, (TOKENS, HEADS * HD), jnp.float32)
    return values.astype(jnp.bfloat16)


def draw_text_key(key, part):
    own_key = jax.random.fold_in(key, 4)
    values = 1.6 * jax.random.truncated_normal(own_key, -4.0, 4.0, (TEXT, HEADS * HD), jnp.float32)
    return values.astype(jnp.bfloat16)


def shard_levels(key, dims, cuts, smallest, top_value):
    gain, own = 1.0, jax.random.fold_in(key, 6)
    for dim, blocks in cuts:
        heights = jnp.exp(jax.random.uniform(jax.random.fold_in(own, dim), (blocks,), jnp.float32, smallest / len(cuts), top_value / len(cuts)))
        gain = gain * jnp.repeat(heights, dims[dim] // blocks).reshape([-1 if axis == dim else 1 for axis in range(len(dims))])
    return gain


def centred(key, shape, scale, reach, cuts=(), kind=jnp.bfloat16):
    values = scale * jax.random.normal(key, shape, jnp.float32)
    if cuts:
        values = values * shard_levels(key, shape, cuts, -0.22, 0.18)
    return jnp.clip(values, -reach, reach).astype(kind)


def setup_inputs(seed: int = 0) -> dict:
    keys = jax.random.split(jax.random.key(seed), 8)
    return {
        "self_query": draw_self_query(jax.random.fold_in(keys[7], 71), 0),
        "self_key": draw_self_key(jax.random.fold_in(keys[7], 71), 0),
        "self_value": centred(keys[2], (TOKENS, HEADS * HD), 1.0, 6.0, ((0, 32),)),
        "cross_query": draw_cross_query(jax.random.fold_in(keys[7], 71), 0),
        "text_key": draw_text_key(jax.random.fold_in(keys[7], 71), 0),
        "text_value": centred(keys[5], (TEXT, HEADS * HD), 1.0, 6.0, ((0, 8), (1, 4))),
        "padded_count": jax.random.randint(keys[6], (1,), 0, TOKENS // 4 + 1).astype(jnp.int32),
    }


neg_fill = -1e+30

def rope_tables(raster, head_size, grid_height, grid_width):
    frame_cells = grid_height * grid_width
    frame_index = raster // frame_cells
    row_index = raster // grid_width % grid_height
    col_index = raster % grid_width
    pair_index = lax.iota(jnp.int32, head_size) // 2
    side_pairs = head_size // 6
    first_pairs = head_size // 2 - 2 * side_pairs
    in_frames = pair_index < first_pairs
    in_rows = pair_index < first_pairs + side_pairs
    numerator = jnp.where(in_frames, pair_index, jnp.where(in_rows, pair_index - first_pairs, pair_index - first_pairs - side_pairs)).astype(jnp.float32)
    denominator = jnp.where(in_frames, first_pairs, side_pairs).astype(jnp.float32)
    omegas = jnp.power(jnp.float32(10000.0), -(numerator / denominator))
    position = jnp.where(in_frames[None, :], frame_index[:, None], jnp.where(in_rows[None, :], row_index[:, None], col_index[:, None])).astype(jnp.float32)
    angles = position * omegas[None, :]
    return (jnp.cos(angles), jnp.sin(angles))

def rotate(values, cosine_table, sine_table):
    channels = values.shape[1]
    repeats = channels // cosine_table.shape[1]
    widened = values.astype(jnp.float32)
    channel = lax.iota(jnp.int32, channels)
    partner = jnp.where(channel % 2 == 0, -jnp.roll(widened, -1, axis=1), jnp.roll(widened, 1, axis=1))
    return (widened * jnp.tile(cosine_table, (1, repeats)) + partner * jnp.tile(sine_table, (1, repeats))).astype(jnp.bfloat16)

def softmax_rows(query_block, key_rows, value_rows, key_mask, scaling):
    scores = jnp.dot(query_block, key_rows.T, preferred_element_type=jnp.float32) * scaling
    if key_mask is not None:
        scores = jnp.where(key_mask[None, :], scores, neg_fill)
    row_peak = lax.optimization_barrier(jnp.max(scores, axis=1, keepdims=True))
    weights = jnp.exp(scores - row_peak)
    totals = lax.optimization_barrier(jnp.sum(weights, axis=1, keepdims=True))
    weighted = jnp.dot(weights.astype(jnp.bfloat16), value_rows, preferred_element_type=jnp.float32)
    return (weighted / totals).astype(jnp.bfloat16)

def attention(queries, keys_all, values_all, key_mask, scaling):
    query_count = queries.shape[0]
    block_rows = 512 if query_count % 512 == 0 else query_count
    block_count = query_count // block_rows
    query_heads = queries.reshape(block_count, block_rows, HEADS, HD).transpose(2, 0, 1, 3)
    key_heads = keys_all.reshape(keys_all.shape[0], HEADS, HD).transpose(1, 0, 2)
    value_heads = values_all.reshape(values_all.shape[0], HEADS, HD).transpose(1, 0, 2)

    def one_head(head_index):

        def one_block(block_index):
            return softmax_rows(query_heads[head_index, block_index], key_heads[head_index], value_heads[head_index], key_mask, scaling)
        return lax.map(one_block, jnp.arange(block_count, dtype=jnp.int32))
    outputs = lax.map(one_head, jnp.arange(HEADS, dtype=jnp.int32))
    return outputs.transpose(1, 2, 0, 3).reshape(query_count, HEADS * HD)

def reference(self_query, self_key, self_value, cross_query, text_key, text_value, padded_count):
    channels = HEADS * HD

    def frame_major(array):
        tile_grid = array.reshape(FRAMES, ROW_TILES, N_ULY, TH, TW, channels)
        return tile_grid.transpose(0, 1, 3, 2, 4, 5).reshape(TOKENS, channels)
    query_rows = frame_major(self_query)
    key_rows = frame_major(self_key)
    value_rows = frame_major(self_value)
    cross_rows = frame_major(cross_query)
    raster = lax.iota(jnp.int32, TOKENS)
    cosine_table, sine_table = rope_tables(raster, HD, GRID_H, GRID_W)
    query_rot = rotate(query_rows, cosine_table, sine_table)
    key_rot = rotate(key_rows, cosine_table, sine_table)
    scaling = 1.0 / math.sqrt(HD)
    key_mask = raster < TOKENS - padded_count[0]
    self_out = attention(query_rot, key_rot, value_rows, key_mask, scaling)
    cross_out = attention(cross_rows, text_key, text_value, None, scaling)
    return (self_out, cross_out)
```

```python
import math

import jax
import jax.numpy as jnp
import numpy as np
from jax import lax
from jax.experimental import pallas as pl
from jax.experimental.pallas import tpu as pltpu
from jax.sharding import PartitionSpec as P

HD = 128
TH = 4
TW = 10
ROW_TILES = 8


neg_fill = -1e30


def rope_tables(raster, head_size, grid_height, grid_width):
    frame_cells = grid_height * grid_width
    frame_index = raster // frame_cells
    row_index = raster // grid_width % grid_height
    col_index = raster % grid_width
    pair_index = lax.iota(jnp.int32, head_size) // 2
    side_pairs = head_size // 6
    first_pairs = head_size // 2 - 2 * side_pairs
    in_frames = pair_index < first_pairs
    in_rows = pair_index < first_pairs + side_pairs
    numerator = jnp.where(
        in_frames,
        pair_index,
        jnp.where(in_rows, pair_index - first_pairs, pair_index - first_pairs - side_pairs),
    ).astype(jnp.float32)
    denominator = jnp.where(in_frames, first_pairs, side_pairs).astype(jnp.float32)
    omegas = jnp.power(jnp.float32(10000.0), -(numerator / denominator))
    position = jnp.where(
        in_frames[None, :],
        frame_index[:, None],
        jnp.where(in_rows[None, :], row_index[:, None], col_index[:, None]),
    ).astype(jnp.float32)
    angles = position * omegas[None, :]
    return (jnp.cos(angles), jnp.sin(angles))


def rotate(values, cosine_table, sine_table):
    channels = values.shape[1]
    repeats = channels // cosine_table.shape[1]
    widened = values.astype(jnp.float32)
    channel = lax.iota(jnp.int32, channels)
    partner = jnp.where(
        channel % 2 == 0, -jnp.roll(widened, -1, axis=1), jnp.roll(widened, 1, axis=1)
    )
    return (
        widened * jnp.tile(cosine_table, (1, repeats))
        + partner * jnp.tile(sine_table, (1, repeats))
    ).astype(jnp.bfloat16)


def block_size(row_count, shard_rows):
    if row_count <= 2048:
        return row_count
    if row_count % 2048 == 0:
        return 2048
    if row_count % 1024 == 0:
        return 1024
    if row_count % 512 == 0:
        return 512
    return shard_rows


def attend_step(current, queries, key_heads, value_heads, key_mask, scaling):
    maxima, totals, accumulated = current
    scores = (
        jnp.einsum("qhd,hkd->qhk", queries, key_heads, preferred_element_type=jnp.float32) * scaling
    )
    if key_mask is not None:
        scores = jnp.where(key_mask[None, None, :], scores, neg_fill)
    new_peak = jnp.maximum(maxima, jnp.max(scores, axis=2))
    weights = jnp.exp(scores - new_peak[:, :, None])
    shrink = jnp.exp(maxima - new_peak)
    totals = totals * shrink + jnp.sum(weights, axis=2)
    accumulated = accumulated * shrink[:, :, None] + jnp.einsum(
        "qhk,hkd->qhd",
        weights.astype(jnp.bfloat16),
        value_heads,
        preferred_element_type=jnp.float32,
    )
    return (new_peak, totals, accumulated)


def attend_rows(current, queries, key_heads, value_heads, key_mask, scaling, shard_rows):
    head_count = key_heads.shape[0]
    row_count = key_heads.shape[1]
    head_size = key_heads.shape[2]
    step_rows = block_size(row_count, shard_rows)
    if step_rows == row_count:
        return attend_step(current, queries, key_heads, value_heads, key_mask, scaling)
    block_count = row_count // step_rows
    key_blocks = key_heads.reshape(head_count, block_count, step_rows, head_size).transpose(
        1, 0, 2, 3
    )
    value_blocks = value_heads.reshape(head_count, block_count, step_rows, head_size).transpose(
        1, 0, 2, 3
    )
    if key_mask is None:

        def advance(carried, blocks):
            return (attend_step(carried, queries, blocks[0], blocks[1], None, scaling), None)

        current, unused = lax.scan(advance, current, (key_blocks, value_blocks))
    else:
        mask_blocks = key_mask.reshape(block_count, step_rows)

        def advance_masked(carried, blocks):
            return (attend_step(carried, queries, blocks[0], blocks[1], blocks[2], scaling), None)

        current, unused = lax.scan(advance_masked, current, (key_blocks, value_blocks, mask_blocks))
    return current


def finish(current):
    maxima, totals, accumulated = current
    return (accumulated / totals[:, :, None]).reshape(accumulated.shape[0], -1).astype(jnp.bfloat16)


def head_major(rows, head_count, head_size):
    return rows.reshape(rows.shape[0], head_count, head_size).transpose(1, 0, 2)


def plain_body(self_query, self_key, self_value, cross_query, text_key, text_value, padded_count):
    blocks_count = lax.axis_size("blk")
    groups_count = lax.axis_size("uly")
    tile_height = TH
    tile_width = TW
    head_size = HD
    channels = self_query.shape[1]
    group_width = channels // groups_count
    head_count = group_width // head_size
    grid_height = tile_height * ROW_TILES
    grid_width = tile_width * groups_count
    shard_rows = tile_height * grid_width
    token_total = blocks_count * shard_rows
    valid_count = token_total - padded_count[0]
    scaling = 1.0 / math.sqrt(head_size)
    block_index = lax.axis_index("blk")
    local_index = lax.iota(jnp.int32, shard_rows)
    shaped_query = self_query.reshape(tile_height, 1, tile_width, channels)
    shaped_key = self_key.reshape(tile_height, 1, tile_width, channels)
    shaped_value = self_value.reshape(tile_height, 1, tile_width, channels)
    shaped_cross = cross_query.reshape(tile_height, 1, tile_width, channels)
    exchanged = (
        lax.all_to_all(shaped_query, "uly", split_axis=3, concat_axis=1, tiled=True),
        lax.all_to_all(shaped_key, "uly", split_axis=3, concat_axis=1, tiled=True),
        lax.all_to_all(shaped_value, "uly", split_axis=3, concat_axis=1, tiled=True),
        lax.all_to_all(shaped_cross, "uly", split_axis=3, concat_axis=1, tiled=True),
    )
    own_raster = block_index * shard_rows + local_index
    cosine_table, sine_table = rope_tables(own_raster, head_size, grid_height, grid_width)
    queries = rotate(
        exchanged[0].reshape(shard_rows, group_width), cosine_table, sine_table
    ).reshape(shard_rows, head_count, head_size)
    keys_local = head_major(
        rotate(exchanged[1].reshape(shard_rows, group_width), cosine_table, sine_table),
        head_count,
        head_size,
    )
    values_local = head_major(exchanged[2].reshape(shard_rows, group_width), head_count, head_size)
    cross_rows = exchanged[3].reshape(shard_rows, head_count, head_size)
    text_keys_heads = head_major(text_key, head_count, head_size)
    text_values_heads = head_major(text_value, head_count, head_size)

    def empty_state():
        return (
            jnp.full((shard_rows, head_count), neg_fill, jnp.float32),
            jnp.zeros((shard_rows, head_count), jnp.float32),
            jnp.zeros((shard_rows, head_count, head_size), jnp.float32),
        )

    pieces = (
        lax.all_gather(keys_local, "blk", axis=1, tiled=True),
        lax.all_gather(values_local, "blk", axis=1, tiled=True),
    )
    key_mask = lax.iota(jnp.int32, pieces[0].shape[1]) < valid_count
    self_state = attend_rows(
        empty_state(), queries, pieces[0], pieces[1], key_mask, scaling, shard_rows
    )
    text_rows = (
        lax.all_gather(text_keys_heads, "blk", axis=1, tiled=True),
        lax.all_gather(text_values_heads, "blk", axis=1, tiled=True),
    )
    cross_state = attend_rows(
        empty_state(), cross_rows, text_rows[0], text_rows[1], None, scaling, text_rows[0].shape[1]
    )
    self_result = finish(self_state)
    cross_result = finish(cross_state)
    token_rows = self_query.shape[0]
    self_grid = self_result.reshape(groups_count, token_rows, 1, group_width)
    cross_grid = cross_result.reshape(groups_count, token_rows, 1, group_width)
    returned = (
        lax.all_to_all(self_grid, "uly", split_axis=0, concat_axis=2, tiled=True),
        lax.all_to_all(cross_grid, "uly", split_axis=0, concat_axis=2, tiled=True),
    )
    return (returned[0].reshape(token_rows, channels), returned[1].reshape(token_rows, channels))


LOG2E = 1.4426950408889634
SMEM = pl.BlockSpec(memory_space=pltpu.SMEM)


def cost(flops, moved):
    return pl.CostEstimate(flops=flops, bytes_accessed=moved, transcendentals=0)


def pack_kernel(uly_ref, x_ref, *outs):
    groups = len(outs)
    width = outs[0].shape[1]
    for k, out in enumerate(outs):
        start = pl.multiple_of((uly_ref[0] + k) % groups * width, width)
        out[...] = x_ref[:, pl.ds(start, width)]


def pack_rotated_kernel(uly_ref, cos_ref, sin_ref, x_ref, *outs):
    groups = len(outs)
    width = outs[0].shape[1]
    head_size = cos_ref.shape[1]
    cosine = cos_ref[...]
    sine = sin_ref[...]
    even = lax.broadcasted_iota(jnp.int32, cosine.shape, 1) % 2 == 0
    for k, out in enumerate(outs):
        start = (uly_ref[0] + k) % groups * width
        for h in range(width // head_size):
            at = pl.multiple_of(start + h * head_size, head_size)
            x = x_ref[:, pl.ds(at, head_size)].astype(jnp.float32)
            partner = jnp.where(even, pltpu.roll(x, head_size - 1, 1), pltpu.roll(x, 1, 1))
            out[:, h * head_size : (h + 1) * head_size] = (x * cosine + partner * sine).astype(jnp.bfloat16)


def pack(x, uly, groups, tables=None):
    rows, channels = x.shape
    shape = jax.ShapeDtypeStruct((rows, channels // groups), x.dtype)
    moved = 2 * x.size * 2
    if tables is None:
        return pl.pallas_call(
            pack_kernel, out_shape=[shape] * groups, in_specs=[SMEM, pl.BlockSpec()],
            cost_estimate=cost(1000, moved), name="pack",
        )(uly, x)
    return pl.pallas_call(
        pack_rotated_kernel, out_shape=[shape] * groups, in_specs=[SMEM] + [pl.BlockSpec()] * 3,
        cost_estimate=cost(1000, moved), name="pack_rotated",
    )(uly, tables[0], tables[1], x)


def merge_kernel(uly_ref, *refs):
    out = refs[-1]
    groups = len(refs) - 1
    rows = refs[0].shape[0]
    for k in range(groups):
        start = pl.multiple_of((uly_ref[0] - k + groups) % groups * rows, rows)
        out[pl.ds(start, rows), :] = refs[k][...]


def merge(chunks, uly):
    rows, width = chunks[0].shape
    return pl.pallas_call(
        merge_kernel, out_shape=jax.ShapeDtypeStruct((len(chunks) * rows, width), chunks[0].dtype),
        in_specs=[SMEM] + [pl.BlockSpec()] * len(chunks),
        cost_estimate=cost(1000, 4 * len(chunks) * rows * width), name="merge",
    )(uly, *chunks)


def unpack_kernel(uly_ref, *refs):
    out = refs[-1]
    groups = len(refs) - 1
    width = refs[0].shape[1]
    for k in range(groups):
        start = pl.multiple_of((uly_ref[0] - k + groups) % groups * width, width)
        out[:, pl.ds(start, width)] = refs[k][...]


def unpack(chunks, uly):
    rows, width = chunks[0].shape
    return pl.pallas_call(
        unpack_kernel, out_shape=jax.ShapeDtypeStruct((rows, len(chunks) * width), chunks[0].dtype),
        in_specs=[SMEM] + [pl.BlockSpec()] * len(chunks),
        cost_estimate=cost(1000, 4 * len(chunks) * rows * width), name="unpack",
    )(uly, *chunks)


def stack_kernel(a_ref, b_ref, out):
    rows = a_ref.shape[0]
    out[:rows, :] = a_ref[...]
    out[rows:, :] = b_ref[...]


def stack(a, b):
    return pl.pallas_call(
        stack_kernel, out_shape=jax.ShapeDtypeStruct((2 * a.shape[0], a.shape[1]), a.dtype),
        cost_estimate=cost(1000, 4 * a.size * 2), name="stack",
    )(a, b)


def attend_kernel(groups, n_keys, split, scaling, *refs):
    place_ref, bias_ref = refs[0], refs[1]
    queries = refs[2 : 2 + groups]
    keys = refs[2 + groups : 2 + groups + n_keys]
    values = refs[2 + groups + n_keys : -groups] if not split else keys
    outs = refs[-groups:]
    rows = queries[0].shape[0]
    q = jnp.concatenate([r[...].astype(jnp.float32) for r in queries], axis=0).astype(jnp.bfloat16)
    q = jnp.dot(place_ref[...], q, preferred_element_type=jnp.float32).astype(jnp.bfloat16)
    if split:
        half = keys[0].shape[0] // 2
        k = jnp.concatenate([r[:half, :] for r in keys], axis=0)
        v = jnp.concatenate([r[half:, :] for r in keys], axis=0)
    else:
        k = jnp.concatenate([r[...] for r in keys], axis=0)
        v = jnp.concatenate([r[...] for r in values], axis=0)
    s = lax.dot_general(q, k, (((1,), (1,)), ((), ())), preferred_element_type=jnp.float32)
    if not split:
        s = s + bias_ref[...]
    m = jnp.max(s, axis=1, keepdims=True)
    p = jnp.exp2((s - m) * (scaling * LOG2E))
    total = jnp.sum(p, axis=1, keepdims=True)
    o = jnp.dot(p.astype(jnp.bfloat16), v, preferred_element_type=jnp.float32) / total
    for i, out in enumerate(outs):
        out[...] = o[i * rows : (i + 1) * rows].astype(jnp.bfloat16)


def attend(place, bias, queries, keys, values, head_size, split, scaling):
    rows, width = queries[0].shape
    groups = len(queries)
    heads = width // head_size
    whole = lambda a: pl.BlockSpec(a.shape, lambda h: (0, 0))
    head = lambda a: pl.BlockSpec((a.shape[0], head_size), lambda h: (0, h))
    parts = list(queries) + list(keys) + list(values)
    n_rows = sum(a.shape[0] for a in keys) // (2 if split else 1)
    return pl.pallas_call(
        lambda *refs: attend_kernel(groups, len(keys), split, scaling, *refs),
        grid=(heads,),
        in_specs=[whole(place), whole(bias)] + [head(a) for a in parts],
        out_specs=[head(a) for a in queries],
        out_shape=[jax.ShapeDtypeStruct((rows, width), queries[0].dtype)] * groups,
        cost_estimate=cost(4 * groups * rows * n_rows * width, 2 * sum(a.size for a in parts)),
        name="attend_cross" if split else "attend_self",
    )(place, bias, *parts)


def swap(x, bit):
    size = lax.axis_size("blk")
    return lax.ppermute(x, "blk", [(i, i ^ bit) for i in range(size)])


def scatter(chunks):
    size = lax.axis_size("uly")
    return [
        c if k == 0 else lax.ppermute(c, "uly", [(i, (i + k) % size) for i in range(size)])
        for k, c in enumerate(chunks)
    ]


def spread(x):
    half = x.shape[0] // 2
    a = swap(x, 2)
    b = swap(x, 4)
    pieces = [x, a, b, swap(a[:half], 4), swap(b[half:], 2)]
    return pieces + [swap(p, 1) for p in pieces]


def cube_body(self_query, self_key, self_value, cross_query, text_key, text_value, padded_count):
    blocks = lax.axis_size("blk")
    groups = lax.axis_size("uly")
    block = lax.axis_index("blk")
    lane = lax.axis_index("uly")
    rows, channels = self_query.shape
    head_size = HD
    shard_rows = rows * groups
    grid_height = TH * ROW_TILES
    grid_width = TW * groups
    scaling = 1.0 / math.sqrt(head_size)
    uly = lane.astype(jnp.int32).reshape(1)
    valid = blocks * shard_rows - padded_count[0]

    n = np.arange(shard_rows)
    tile, i, j = n // rows, n % rows // TW, n % TW
    offset = i * grid_width + tile * TW + j
    own = block * shard_rows + jnp.asarray(offset[:rows], jnp.int32) + lane * TW
    cosine, sine = rope_tables(own, head_size, grid_height, grid_width)
    sine = sine * jnp.where(lax.iota(jnp.int32, head_size) % 2 == 0, -1.0, 1.0)[None, :]
    tables = (cosine, sine)

    value_chunks = scatter(pack(self_value, uly, groups))
    key_chunks = scatter(pack(self_key, uly, groups, tables))
    text = stack(text_key, text_value)
    text_pieces = [text, swap(text, 2), swap(text, 4), swap(text, 6)]
    text_pieces = text_pieces + [swap(t, 1) for t in text_pieces]
    values = spread(merge(value_chunks, uly))
    keys = spread(merge(key_chunks, uly))
    cross_chunks = scatter(pack(cross_query, uly, groups))
    query_chunks = scatter(pack(self_query, uly, groups, tables))

    r = lax.iota(jnp.int32, shard_rows)
    source = (lane - r % rows // TW + groups) % groups * rows + (lane + r // rows) % groups * TW + r % TW
    place = (source[:, None] == r[None, :]).astype(jnp.bfloat16)
    half = shard_rows // 2
    spans = [(0, 0, shard_rows), (2, 0, shard_rows), (4, 0, shard_rows), (6, 0, half), (6, half, shard_rows)]
    spans = spans + [(m ^ 1, lo, hi) for m, lo, hi in spans]
    where = jnp.concatenate([(block ^ m) * shard_rows + jnp.asarray(offset[lo:hi], jnp.int32) for m, lo, hi in spans])
    bias = jnp.where(where < valid, 0.0, neg_fill).astype(jnp.float32)[None, :]

    cross = attend(place, bias, cross_chunks, text_pieces, [], head_size, True, scaling)
    cross_back = scatter(cross)
    selfs = attend(place, bias, query_chunks, keys, values, head_size, False, scaling)
    self_back = scatter(selfs)
    return unpack(self_back, uly), unpack(cross_back, uly)


def body(*args):
    rows = args[0].shape[0]
    fits = lax.axis_size("blk") * lax.axis_size("uly") * rows <= 2048
    if lax.axis_size("blk") == 8 and lax.axis_size("uly") == TH and fits:
        return cube_body(*args)
    return plain_body(*args)


def solution(mesh):
    in_specs = (
        P(("blk", "uly"), None),
        P(("blk", "uly"), None),
        P(("blk", "uly"), None),
        P(("blk", "uly"), None),
        P("blk", "uly"),
        P("blk", "uly"),
        P(),
    )
    out_specs = (P(("blk", "uly"), None), P(("blk", "uly"), None))
    return jax.shard_map(body, mesh=mesh, in_specs=in_specs, out_specs=out_specs, check_vma=False)
```

```python
import math

import jax
import jax.numpy as jnp
import numpy as np
from jax import lax
from jax.experimental import pallas as pl
from jax.experimental.pallas import tpu as pltpu
from jax.sharding import PartitionSpec as P

HD = 128
TH = 4
TW = 10
ROW_TILES = 8


neg_fill = -1e30


def rope_tables(raster, head_size, grid_height, grid_width):
    frame_cells = grid_height * grid_width
    frame_index = raster // frame_cells
    row_index = raster // grid_width % grid_height
    col_index = raster % grid_width
    pair_index = lax.iota(jnp.int32, head_size) // 2
    side_pairs = head_size // 6
    first_pairs = head_size // 2 - 2 * side_pairs
    in_frames = pair_index < first_pairs
    in_rows = pair_index < first_pairs + side_pairs
    numerator = jnp.where(
        in_frames,
        pair_index,
        jnp.where(in_rows, pair_index - first_pairs, pair_index - first_pairs - side_pairs),
    ).astype(jnp.float32)
    denominator = jnp.where(in_frames, first_pairs, side_pairs).astype(jnp.float32)
    omegas = jnp.power(jnp.float32(10000.0), -(numerator / denominator))
    position = jnp.where(
        in_frames[None, :],
        frame_index[:, None],
        jnp.where(in_rows[None, :], row_index[:, None], col_index[:, None]),
    ).astype(jnp.float32)
    angles = position * omegas[None, :]
    return (jnp.cos(angles), jnp.sin(angles))


def rotate(values, cosine_table, sine_table):
    channels = values.shape[1]
    repeats = channels // cosine_table.shape[1]
    widened = values.astype(jnp.float32)
    channel = lax.iota(jnp.int32, channels)
    partner = jnp.where(
        channel % 2 == 0, -jnp.roll(widened, -1, axis=1), jnp.roll(widened, 1, axis=1)
    )
    return (
        widened * jnp.tile(cosine_table, (1, repeats))
        + partner * jnp.tile(sine_table, (1, repeats))
    ).astype(jnp.bfloat16)


def block_size(row_count, shard_rows):
    if row_count <= 2048:
        return row_count
    if row_count % 2048 == 0:
        return 2048
    if row_count % 1024 == 0:
        return 1024
    if row_count % 512 == 0:
        return 512
    return shard_rows


def attend_step(current, queries, key_heads, value_heads, key_mask, scaling):
    maxima, totals, accumulated = current
    scores = (
        jnp.einsum("qhd,hkd->qhk", queries, key_heads, preferred_element_type=jnp.float32) * scaling
    )
    if key_mask is not None:
        scores = jnp.where(key_mask[None, None, :], scores, neg_fill)
    new_peak = jnp.maximum(maxima, jnp.max(scores, axis=2))
    weights = jnp.exp(scores - new_peak[:, :, None])
    shrink = jnp.exp(maxima - new_peak)
    totals = totals * shrink + jnp.sum(weights, axis=2)
    accumulated = accumulated * shrink[:, :, None] + jnp.einsum(
        "qhk,hkd->qhd",
        weights.astype(jnp.bfloat16),
        value_heads,
        preferred_element_type=jnp.float32,
    )
    return (new_peak, totals, accumulated)


def attend_rows(current, queries, key_heads, value_heads, key_mask, scaling, shard_rows):
    head_count = key_heads.shape[0]
    row_count = key_heads.shape[1]
    head_size = key_heads.shape[2]
    step_rows = block_size(row_count, shard_rows)
    if step_rows == row_count:
        return attend_step(current, queries, key_heads, value_heads, key_mask, scaling)
    block_count = row_count // step_rows
    key_blocks = key_heads.reshape(head_count, block_count, step_rows, head_size).transpose(
        1, 0, 2, 3
    )
    value_blocks = value_heads.reshape(head_count, block_count, step_rows, head_size).transpose(
        1, 0, 2, 3
    )
    if key_mask is None:

        def advance(carried, blocks):
            return (attend_step(carried, queries, blocks[0], blocks[1], None, scaling), None)

        current, unused = lax.scan(advance, current, (key_blocks, value_blocks))
    else:
        mask_blocks = key_mask.reshape(block_count, step_rows)

        def advance_masked(carried, blocks):
            return (attend_step(carried, queries, blocks[0], blocks[1], blocks[2], scaling), None)

        current, unused = lax.scan(advance_masked, current, (key_blocks, value_blocks, mask_blocks))
    return current


def finish(current):
    maxima, totals, accumulated = current
    return (accumulated / totals[:, :, None]).reshape(accumulated.shape[0], -1).astype(jnp.bfloat16)


def head_major(rows, head_count, head_size):
    return rows.reshape(rows.shape[0], head_count, head_size).transpose(1, 0, 2)


def plain_body(self_query, self_key, self_value, cross_query, text_key, text_value, padded_count):
    blocks_count = lax.axis_size("blk")
    groups_count = lax.axis_size("uly")
    tile_height = TH
    tile_width = TW
    head_size = HD
    channels = self_query.shape[1]
    group_width = channels // groups_count
    head_count = group_width // head_size
    grid_height = tile_height * ROW_TILES
    grid_width = tile_width * groups_count
    shard_rows = tile_height * grid_width
    token_total = blocks_count * shard_rows
    valid_count = token_total - padded_count[0]
    scaling = 1.0 / math.sqrt(head_size)
    block_index = lax.axis_index("blk")
    local_index = lax.iota(jnp.int32, shard_rows)
    shaped_query = self_query.reshape(tile_height, 1, tile_width, channels)
    shaped_key = self_key.reshape(tile_height, 1, tile_width, channels)
    shaped_value = self_value.reshape(tile_height, 1, tile_width, channels)
    shaped_cross = cross_query.reshape(tile_height, 1, tile_width, channels)
    exchanged = (
        lax.all_to_all(shaped_query, "uly", split_axis=3, concat_axis=1, tiled=True),
        lax.all_to_all(shaped_key, "uly", split_axis=3, concat_axis=1, tiled=True),
        lax.all_to_all(shaped_value, "uly", split_axis=3, concat_axis=1, tiled=True),
        lax.all_to_all(shaped_cross, "uly", split_axis=3, concat_axis=1, tiled=True),
    )
    own_raster = block_index * shard_rows + local_index
    cosine_table, sine_table = rope_tables(own_raster, head_size, grid_height, grid_width)
    queries = rotate(
        exchanged[0].reshape(shard_rows, group_width), cosine_table, sine_table
    ).reshape(shard_rows, head_count, head_size)
    keys_local = head_major(
        rotate(exchanged[1].reshape(shard_rows, group_width), cosine_table, sine_table),
        head_count,
        head_size,
    )
    values_local = head_major(exchanged[2].reshape(shard_rows, group_width), head_count, head_size)
    cross_rows = exchanged[3].reshape(shard_rows, head_count, head_size)
    text_keys_heads = head_major(text_key, head_count, head_size)
    text_values_heads = head_major(text_value, head_count, head_size)

    def empty_state():
        return (
            jnp.full((shard_rows, head_count), neg_fill, jnp.float32),
            jnp.zeros((shard_rows, head_count), jnp.float32),
            jnp.zeros((shard_rows, head_count, head_size), jnp.float32),
        )

    pieces = (
        lax.all_gather(keys_local, "blk", axis=1, tiled=True),
        lax.all_gather(values_local, "blk", axis=1, tiled=True),
    )
    key_mask = lax.iota(jnp.int32, pieces[0].shape[1]) < valid_count
    self_state = attend_rows(
        empty_state(), queries, pieces[0], pieces[1], key_mask, scaling, shard_rows
    )
    text_rows = (
        lax.all_gather(text_keys_heads, "blk", axis=1, tiled=True),
        lax.all_gather(text_values_heads, "blk", axis=1, tiled=True),
    )
    cross_state = attend_rows(
        empty_state(), cross_rows, text_rows[0], text_rows[1], None, scaling, text_rows[0].shape[1]
    )
    self_result = finish(self_state)
    cross_result = finish(cross_state)
    token_rows = self_query.shape[0]
    self_grid = self_result.reshape(groups_count, token_rows, 1, group_width)
    cross_grid = cross_result.reshape(groups_count, token_rows, 1, group_width)
    returned = (
        lax.all_to_all(self_grid, "uly", split_axis=0, concat_axis=2, tiled=True),
        lax.all_to_all(cross_grid, "uly", split_axis=0, concat_axis=2, tiled=True),
    )
    return (returned[0].reshape(token_rows, channels), returned[1].reshape(token_rows, channels))


LOG2E = 1.4426950408889634
SMEM = pl.BlockSpec(memory_space=pltpu.SMEM)
WHOLE = pl.BlockSpec()
UNREAD = pl.BlockSpec(memory_space=pl.ANY)
MIB = 1 << 20


def call(kernel, name, outs, args, scalars, after=(), limit=2, flops=1000):
    def run(*refs):
        k = 1 + len(args)
        kernel(refs[0], refs[1:k], refs[k + len(after) :])

    return pl.pallas_call(
        run,
        out_shape=outs,
        in_specs=[SMEM] + [WHOLE] * len(args) + [UNREAD] * len(after),
        compiler_params=pltpu.CompilerParams(vmem_limit_bytes=limit * MIB),
        cost_estimate=pl.CostEstimate(flops=flops, bytes_accessed=4 * sum(a.size for a in args), transcendentals=0),
        name=name,
    )(scalars, *args, *after)


def copy_chunks(uly, x, outs, at):
    rows = x.shape[0]
    width = outs[0].shape[1]
    for k, out in enumerate(outs):
        start = pl.multiple_of((uly ^ k) * width, width)
        out[at : at + rows, :] = x[:, pl.ds(start, width)]


def rotate_chunks(uly, block, omega, x, outs, at, grid_width):
    rows = x.shape[0]
    width = outs[0].shape[1]
    head_size = omega.shape[1]
    side = head_size // 6
    first = head_size // 2 - 2 * side
    shape = (rows, head_size)
    token = lax.broadcasted_iota(jnp.int32, shape, 0)
    channel = lax.broadcasted_iota(jnp.int32, shape, 1)
    pair = channel // 2
    frame = block // ROW_TILES + jnp.zeros(shape, jnp.int32)
    row = block % ROW_TILES * TH + token // TW
    col = uly * TW + token % TW
    position = jnp.where(pair < first, frame, jnp.where(pair < first + side, row, col))
    angle = position.astype(jnp.float32) * omega[...]
    even = channel % 2 == 0
    cosine = jnp.cos(angle)
    sine = jnp.where(even, -1.0, 1.0) * jnp.sin(angle)
    for k, out in enumerate(outs):
        start = (uly ^ k) * width
        for h in range(width // head_size):
            place = pl.multiple_of(start + h * head_size, head_size)
            v = x[:, pl.ds(place, head_size)].astype(jnp.float32)
            partner = jnp.where(even, pltpu.roll(v, head_size - 1, 1), pltpu.roll(v, 1, 1))
            turned = (v * cosine + partner * sine).astype(jnp.bfloat16)
            out[at : at + rows, h * head_size : (h + 1) * head_size] = turned


def attend_kernel(where, args, outs, chunks, pieces, split, scaling, head_size):
    place, bias = args[0], args[1]
    queries = args[2 : 2 + chunks]
    keys = args[2 + chunks : 2 + chunks + pieces]
    values = args[2 + chunks + pieces :]
    rows = outs[0].shape[0]
    at = rows if not split else 0
    width = outs[0].shape[1]

    def one_head(h, carry):
        cols = pl.ds(pl.multiple_of(h * head_size, head_size), head_size)
        q = jnp.concatenate([r[at : at + rows, cols].astype(jnp.float32) for r in queries], axis=0)
        q = jnp.dot(place[...], q.astype(jnp.bfloat16), preferred_element_type=jnp.float32).astype(jnp.bfloat16)
        if split:
            full = keys[0].shape[0]
            n = full // 2
            halves = [r for r in keys if r.shape[0] == n]
            k = [r[:n, cols] for r in keys if r.shape[0] == full] + [r[:, cols] for r in halves[::2]]
            v = [r[n:, cols] for r in keys if r.shape[0] == full] + [r[:, cols] for r in halves[1::2]]
            k = jnp.concatenate(k, axis=0)
            v = jnp.concatenate(v, axis=0)
        else:
            k = jnp.concatenate([r[:, cols] for r in keys], axis=0)
            v = jnp.concatenate([r[:, cols] for r in values], axis=0)
        s = lax.dot_general(q, k, (((1,), (1,)), ((), ())), preferred_element_type=jnp.float32)
        if not split:
            s = s + bias[...]
        m = jnp.max(s, axis=1, keepdims=True)
        p = jnp.exp2((s - m) * (scaling * LOG2E))
        total = jnp.sum(p, axis=1, keepdims=True)
        o = jnp.dot(p.astype(jnp.bfloat16), v, preferred_element_type=jnp.float32) / total
        for i, out in enumerate(outs):
            out[:, cols] = o[i * rows : (i + 1) * rows].astype(jnp.bfloat16)
        return carry

    lax.fori_loop(0, width // head_size, one_head, 0, unroll=2)


def attend(where, place, bias, queries, keys, values, split, scaling):
    rows = place.shape[0] // len(queries)
    width = queries[0].shape[1]
    args = [place, bias] + list(queries) + list(keys) + list(values)
    kernel = lambda s, a, o: attend_kernel(s, a, o, len(queries), len(keys), split, scaling, HD)
    seen = sum(a.size for a in keys) // (2 if split else 1)
    return call(
        kernel, "attend_cross" if split else "attend_self",
        [jax.ShapeDtypeStruct((rows, width), jnp.bfloat16)] * len(queries), args, where,
        limit=8 if split else 16, flops=4 * place.shape[0] * seen,
    )


def swap(x, bit):
    size = lax.axis_size("blk")
    return lax.ppermute(x, "blk", [(i, i ^ bit) for i in range(size)])


def scatter(chunks):
    size = lax.axis_size("uly")
    return [c if k == 0 else lax.ppermute(c, "uly", [(i, i ^ k) for i in range(size)]) for k, c in enumerate(chunks)]


def spread(x):
    half = x.shape[0] // 2
    a = swap(x, 2)
    b = swap(x, 4)
    pieces = [x, a, b, swap(a[:half], 4), swap(b[half:], 2)]
    return pieces + [swap(p, 1) for p in pieces]


def cube_body(self_query, self_key, self_value, cross_query, text_key, text_value, padded_count):
    blocks = lax.axis_size("blk")
    groups = lax.axis_size("uly")
    block = lax.axis_index("blk")
    lane = lax.axis_index("uly")
    rows, channels = self_query.shape
    width = channels // groups
    shard_rows = rows * groups
    grid_width = TW * groups
    scaling = 1.0 / math.sqrt(HD)
    where = jnp.stack([lane, block]).astype(jnp.int32)
    valid = blocks * shard_rows - padded_count[0]

    side = HD // 6
    first = HD // 2 - 2 * side
    pair = np.arange(HD) // 2
    bands = [pair < first, pair < first + side]
    step = np.select(bands, [pair / first, (pair - first) / side], (pair - first - side) / side)
    omega = jnp.asarray(10000.0**-step, jnp.float32)[None, :]

    shape = lambda n, w=width: jax.ShapeDtypeStruct((n, w), jnp.bfloat16)

    def pack_values(s, a, o):
        copy_chunks(s[0], a[0], o, 0)

    def pack_keys(s, a, o):
        rotate_chunks(s[0], s[1], a[0], a[1], o[:groups], 0, grid_width)
        n = a[2].shape[0]
        o[groups][:n, :] = a[2][...]
        o[groups][n:, :] = a[3][...]

    def pack_queries(s, a, o):
        copy_chunks(s[0], a[2], o, 0)
        rotate_chunks(s[0], s[1], a[0], a[1], o, rows, grid_width)

    def merge_chunks(s, a, o):
        for k, chunk in enumerate(a):
            start = pl.multiple_of((s[0] ^ k) * rows, rows)
            o[0][pl.ds(start, rows), :] = chunk[...]

    def unpack_chunks(s, a, o):
        for k, chunk in enumerate(a):
            start = pl.multiple_of((s[0] ^ k) * width, width)
            o[0][:, pl.ds(start, width)] = chunk[...]

    def merge(chunks):
        return call(merge_chunks, "merge", [shape(shard_rows)], chunks, where)[0]

    def unpack(chunks):
        return call(unpack_chunks, "unpack", [shape(rows, channels)], chunks, where)[0]

    value_chunks = scatter(call(pack_values, "pack_values", [shape(rows)] * groups, [self_value], where))
    packed = call(
        pack_keys, "pack_keys", [shape(rows)] * groups + [shape(2 * text_key.shape[0])],
        [omega, self_key, text_key, text_value], where,
    )
    key_chunks = scatter(packed[:groups])
    text = spread(packed[groups])
    merged = merge(value_chunks)
    values = spread(merged)
    packed = call(
        pack_queries, "pack_queries", [shape(2 * rows)] * groups, [omega, self_query, cross_query], where,
        after=[merged], limit=4,
    )
    query_chunks = scatter(packed)
    keys = spread(merge(key_chunks))

    n = np.arange(shard_rows)
    offset = n % rows // TW * grid_width + n // rows * TW + n % TW
    r = lax.iota(jnp.int32, shard_rows)
    source = (lane ^ (r % rows // TW)) * rows + (lane ^ (r // rows)) * TW + r % TW
    place = (source[:, None] == r[None, :]).astype(jnp.bfloat16)
    half = shard_rows // 2
    spans = [(0, 0, shard_rows), (2, 0, shard_rows), (4, 0, shard_rows), (6, 0, half), (6, half, shard_rows)]
    spans = spans + [(m ^ 1, lo, hi) for m, lo, hi in spans]
    owner = np.concatenate([np.full(hi - lo, m) for m, lo, hi in spans])
    inside = np.concatenate([offset[lo:hi] for m, lo, hi in spans])
    position = (block ^ jnp.asarray(owner, jnp.int32)) * shard_rows + jnp.asarray(inside, jnp.int32)
    bias = jnp.where(position < valid, 0.0, neg_fill).astype(jnp.float32)[None, :]

    cross_back = scatter(attend(where, place, bias, query_chunks, text, [], True, scaling))
    self_back = scatter(attend(where, place, bias, query_chunks, keys, values, False, scaling))
    return unpack(self_back), unpack(cross_back)


def body(*args):
    rows = args[0].shape[0]
    fits = lax.axis_size("blk") * lax.axis_size("uly") * rows <= 2048
    if lax.axis_size("blk") == 8 and lax.axis_size("uly") == TH and fits:
        return cube_body(*args)
    return plain_body(*args)


def solution(mesh):
    in_specs = (
        P(("blk", "uly"), None),
        P(("blk", "uly"), None),
        P(("blk", "uly"), None),
        P(("blk", "uly"), None),
        P("blk", "uly"),
        P("blk", "uly"),
        P(),
    )
    out_specs = (P(("blk", "uly"), None), P(("blk", "uly"), None))
    return jax.shard_map(body, mesh=mesh, in_specs=in_specs, out_specs=out_specs, check_vma=False)
```

```python
import math

import jax
import jax.numpy as jnp
import numpy as np
from jax import lax
from jax.experimental import pallas as pl
from jax.experimental.pallas import tpu as pltpu
from jax.sharding import PartitionSpec as P


HD = 128
TH = 4
TW = 10
ROW_TILES = 8


neg_fill = -1e30


def rope_tables(raster, head_size, grid_height, grid_width):
    frame_cells = grid_height * grid_width
    frame_index = raster // frame_cells
    row_index = raster // grid_width % grid_height
    col_index = raster % grid_width
    pair_index = lax.iota(jnp.int32, head_size) // 2
    side_pairs = head_size // 6
    first_pairs = head_size // 2 - 2 * side_pairs
    in_frames = pair_index < first_pairs
    in_rows = pair_index < first_pairs + side_pairs
    numerator = jnp.where(
        in_frames,
        pair_index,
        jnp.where(in_rows, pair_index - first_pairs, pair_index - first_pairs - side_pairs),
    ).astype(jnp.float32)
    denominator = jnp.where(in_frames, first_pairs, side_pairs).astype(jnp.float32)
    omegas = jnp.power(jnp.float32(10000.0), -(numerator / denominator))
    position = jnp.where(
        in_frames[None, :],
        frame_index[:, None],
        jnp.where(in_rows[None, :], row_index[:, None], col_index[:, None]),
    ).astype(jnp.float32)
    angles = position * omegas[None, :]
    return (jnp.cos(angles), jnp.sin(angles))


def rotate(values, cosine_table, sine_table):
    channels = values.shape[1]
    repeats = channels // cosine_table.shape[1]
    widened = values.astype(jnp.float32)
    channel = lax.iota(jnp.int32, channels)
    partner = jnp.where(
        channel % 2 == 0, -jnp.roll(widened, -1, axis=1), jnp.roll(widened, 1, axis=1)
    )
    return (
        widened * jnp.tile(cosine_table, (1, repeats))
        + partner * jnp.tile(sine_table, (1, repeats))
    ).astype(jnp.bfloat16)


def block_size(row_count, shard_rows):
    if row_count <= 2048:
        return row_count
    if row_count % 2048 == 0:
        return 2048
    if row_count % 1024 == 0:
        return 1024
    if row_count % 512 == 0:
        return 512
    return shard_rows


def attend_step(current, queries, key_heads, value_heads, key_mask, scaling):
    maxima, totals, accumulated = current
    scores = (
        jnp.einsum("qhd,hkd->qhk", queries, key_heads, preferred_element_type=jnp.float32) * scaling
    )
    if key_mask is not None:
        scores = jnp.where(key_mask[None, None, :], scores, neg_fill)
    new_peak = jnp.maximum(maxima, jnp.max(scores, axis=2))
    weights = jnp.exp(scores - new_peak[:, :, None])
    shrink = jnp.exp(maxima - new_peak)
    totals = totals * shrink + jnp.sum(weights, axis=2)
    accumulated = accumulated * shrink[:, :, None] + jnp.einsum(
        "qhk,hkd->qhd",
        weights.astype(jnp.bfloat16),
        value_heads,
        preferred_element_type=jnp.float32,
    )
    return (new_peak, totals, accumulated)


def attend_rows(current, queries, key_heads, value_heads, key_mask, scaling, shard_rows):
    head_count = key_heads.shape[0]
    row_count = key_heads.shape[1]
    head_size = key_heads.shape[2]
    step_rows = block_size(row_count, shard_rows)
    if step_rows == row_count:
        return attend_step(current, queries, key_heads, value_heads, key_mask, scaling)
    block_count = row_count // step_rows
    key_blocks = key_heads.reshape(head_count, block_count, step_rows, head_size).transpose(
        1, 0, 2, 3
    )
    value_blocks = value_heads.reshape(head_count, block_count, step_rows, head_size).transpose(
        1, 0, 2, 3
    )
    if key_mask is None:

        def advance(carried, blocks):
            return (attend_step(carried, queries, blocks[0], blocks[1], None, scaling), None)

        current, unused = lax.scan(advance, current, (key_blocks, value_blocks))
    else:
        mask_blocks = key_mask.reshape(block_count, step_rows)

        def advance_masked(carried, blocks):
            return (attend_step(carried, queries, blocks[0], blocks[1], blocks[2], scaling), None)

        current, unused = lax.scan(advance_masked, current, (key_blocks, value_blocks, mask_blocks))
    return current


def finish(current):
    _, totals, accumulated = current
    return (accumulated / totals[:, :, None]).reshape(accumulated.shape[0], -1).astype(jnp.bfloat16)


def head_major(rows, head_count, head_size):
    return rows.reshape(rows.shape[0], head_count, head_size).transpose(1, 0, 2)


def plain_body(self_query, self_key, self_value, cross_query, text_key, text_value, padded_count):
    blocks_count = lax.axis_size("blk")
    groups_count = lax.axis_size("uly")
    tile_height = TH
    tile_width = TW
    head_size = HD
    channels = self_query.shape[1]
    group_width = channels // groups_count
    head_count = group_width // head_size
    grid_height = tile_height * ROW_TILES
    grid_width = tile_width * groups_count
    shard_rows = tile_height * grid_width
    token_total = blocks_count * shard_rows
    valid_count = token_total - padded_count[0]
    scaling = 1.0 / math.sqrt(head_size)
    block_index = lax.axis_index("blk")
    local_index = lax.iota(jnp.int32, shard_rows)
    shaped_query = self_query.reshape(tile_height, 1, tile_width, channels)
    shaped_key = self_key.reshape(tile_height, 1, tile_width, channels)
    shaped_value = self_value.reshape(tile_height, 1, tile_width, channels)
    shaped_cross = cross_query.reshape(tile_height, 1, tile_width, channels)
    exchanged = (
        lax.all_to_all(shaped_query, "uly", split_axis=3, concat_axis=1, tiled=True),
        lax.all_to_all(shaped_key, "uly", split_axis=3, concat_axis=1, tiled=True),
        lax.all_to_all(shaped_value, "uly", split_axis=3, concat_axis=1, tiled=True),
        lax.all_to_all(shaped_cross, "uly", split_axis=3, concat_axis=1, tiled=True),
    )
    own_raster = block_index * shard_rows + local_index
    cosine_table, sine_table = rope_tables(own_raster, head_size, grid_height, grid_width)
    queries = rotate(
        exchanged[0].reshape(shard_rows, group_width), cosine_table, sine_table
    ).reshape(shard_rows, head_count, head_size)
    keys_local = head_major(
        rotate(exchanged[1].reshape(shard_rows, group_width), cosine_table, sine_table),
        head_count,
        head_size,
    )
    values_local = head_major(exchanged[2].reshape(shard_rows, group_width), head_count, head_size)
    cross_rows = exchanged[3].reshape(shard_rows, head_count, head_size)
    text_keys_heads = head_major(text_key, head_count, head_size)
    text_values_heads = head_major(text_value, head_count, head_size)

    def empty_state():
        return (
            jnp.full((shard_rows, head_count), neg_fill, jnp.float32),
            jnp.zeros((shard_rows, head_count), jnp.float32),
            jnp.zeros((shard_rows, head_count, head_size), jnp.float32),
        )

    pieces = (
        lax.all_gather(keys_local, "blk", axis=1, tiled=True),
        lax.all_gather(values_local, "blk", axis=1, tiled=True),
    )
    key_mask = lax.iota(jnp.int32, pieces[0].shape[1]) < valid_count
    self_state = attend_rows(
        empty_state(), queries, pieces[0], pieces[1], key_mask, scaling, shard_rows
    )
    text_rows = (
        lax.all_gather(text_keys_heads, "blk", axis=1, tiled=True),
        lax.all_gather(text_values_heads, "blk", axis=1, tiled=True),
    )
    cross_state = attend_rows(
        empty_state(), cross_rows, text_rows[0], text_rows[1], None, scaling, text_rows[0].shape[1]
    )
    self_result = finish(self_state)
    cross_result = finish(cross_state)
    token_rows = self_query.shape[0]
    self_grid = self_result.reshape(groups_count, token_rows, 1, group_width)
    cross_grid = cross_result.reshape(groups_count, token_rows, 1, group_width)
    returned = (
        lax.all_to_all(self_grid, "uly", split_axis=0, concat_axis=2, tiled=True),
        lax.all_to_all(cross_grid, "uly", split_axis=0, concat_axis=2, tiled=True),
    )
    return (returned[0].reshape(token_rows, channels), returned[1].reshape(token_rows, channels))


LOG2E = 1.4426950408889634
SMEM = pl.BlockSpec(memory_space=pltpu.SMEM)
WHOLE = pl.BlockSpec()
UNREAD = pl.BlockSpec(memory_space=pl.ANY)
MIB = 1 << 20


def call(kernel, outs, args, scalars, after=(), limit=2, flops=1000):
    def run(*refs):
        k = 1 + len(args)
        kernel(refs[0], refs[1:k], refs[k + len(after) :])

    return pl.pallas_call(
        run,
        out_shape=outs,
        in_specs=[SMEM] + [WHOLE] * len(args) + [UNREAD] * len(after),
        compiler_params=pltpu.CompilerParams(vmem_limit_bytes=limit * MIB),
        cost_estimate=pl.CostEstimate(flops=flops, bytes_accessed=4 * sum(a.size for a in args), transcendentals=0),
    )(scalars, *args, *after)


def copy_chunks(uly, x, outs, at):
    rows = x.shape[0]
    width = outs[0].shape[1]
    for k, out in enumerate(outs):
        start = pl.multiple_of((uly ^ k) * width, width)
        out[at : at + rows, :] = x[:, pl.ds(start, width)]


def rotate_chunks(uly, block, omega, x, outs, at):
    rows = x.shape[0]
    width = outs[0].shape[1]
    head_size = omega.shape[1]
    side = head_size // 6
    first = head_size // 2 - 2 * side
    shape = (rows, head_size)
    token = lax.broadcasted_iota(jnp.int32, shape, 0)
    channel = lax.broadcasted_iota(jnp.int32, shape, 1)
    pair = channel // 2
    frame = block // ROW_TILES + jnp.zeros(shape, jnp.int32)
    row = block % ROW_TILES * TH + token // TW
    col = uly * TW + token % TW
    position = jnp.where(pair < first, frame, jnp.where(pair < first + side, row, col))
    angle = position.astype(jnp.float32) * omega[...]
    even = channel % 2 == 0
    cosine = jnp.cos(angle)
    sine = jnp.where(even, -1.0, 1.0) * jnp.sin(angle)
    for k, out in enumerate(outs):
        start = (uly ^ k) * width
        for h in range(width // head_size):
            place = pl.multiple_of(start + h * head_size, head_size)
            v = x[:, pl.ds(place, head_size)].astype(jnp.float32)
            partner = jnp.where(even, pltpu.roll(v, head_size - 1, 1), pltpu.roll(v, 1, 1))
            turned = (v * cosine + partner * sine).astype(jnp.bfloat16)
            out[at : at + rows, h * head_size : (h + 1) * head_size] = turned


def place_rows(place, chunks, start, out):
    for h in range(0, out.shape[1], HD):
        cols = pl.ds(pl.multiple_of(start + h, HD), HD)
        q = jnp.concatenate([r[:, cols].astype(jnp.float32) for r in chunks], axis=0).astype(jnp.bfloat16)
        out[:, h : h + HD] = jnp.dot(place[...], q, preferred_element_type=jnp.float32).astype(jnp.bfloat16)


def attend_kernel(queries, bias, keys, values, outs, split, scaling, head_size):
    rows = outs[0].shape[0]
    heads = outs[0].shape[1] // head_size

    def load(h):
        cols = slice(h * head_size, (h + 1) * head_size)
        if split:
            n = keys[0].shape[0] // 2
            k = [r[:n, cols] for r in keys]
            v = [r[n:, cols] for r in keys]
        else:
            k = [r[:, cols] for r in keys]
            v = [r[:, cols] for r in values]
        k = jnp.concatenate(k, axis=0)
        s = lax.dot_general(queries[:, cols], k, (((1,), (1,)), ((), ())), preferred_element_type=jnp.float32)
        return (s if split else s + bias[...]), jnp.concatenate(v, axis=0)

    s, v = load(0)
    for h in range(heads):
        ahead = load(h + 1) if h + 1 < heads else (None, None)
        m = jnp.max(s, axis=1, keepdims=True)
        p = jnp.exp2((s - m) * (scaling * LOG2E))
        total = jnp.sum(p, axis=1, keepdims=True)
        o = jnp.dot(p.astype(jnp.bfloat16), v, preferred_element_type=jnp.float32) / total
        for k, out in enumerate(outs):
            out[:, h * head_size : (h + 1) * head_size] = o[k * rows : (k + 1) * rows].astype(jnp.bfloat16)
        s, v = ahead


def attend(where, place, queries, bias, keys, values, groups, width, split, scaling):
    rows = sum(q.shape[0] for q in queries)
    args = ([place] if place is not None else []) + list(queries) + [bias] + list(keys) + list(values)

    def kernel(s, a, o):
        at = len(args) - len(keys) - len(values) - 1
        q = a[0]
        if place is not None:
            q = o[groups]
            place_rows(a[0], a[1:at], s[2] * width if width < a[1].shape[1] else 0, q)
        ends = at + 1 + len(keys)
        attend_kernel(q, a[at], a[at + 1 : ends], a[ends:], o[:groups], split, scaling, HD)

    outs = [jax.ShapeDtypeStruct((rows // groups, width), jnp.bfloat16)] * groups
    ordered = [jax.ShapeDtypeStruct((rows, width), jnp.bfloat16)] if place is not None else []
    seen = sum(a.size for a in keys) // (2 if split else 1)
    return call(kernel, outs + ordered, args, where, limit=16, flops=4 * rows * seen)[:groups]


def swap(x, bit):
    size = lax.axis_size("blk")
    return lax.ppermute(x, "blk", [(i, i ^ bit) for i in range(size)])


def scatter(chunks):
    size = lax.axis_size("uly")
    out = [chunks[0]]
    for k, c in enumerate(chunks[1:], 1):
        out.append(lax.ppermute(c, "uly", [(i, i ^ k) for i in range(size)]))
    return out


def spread(x):
    far = swap(x, 4)
    pieces = [x, swap(x, 2), far, swap(far, 2)]
    return pieces + [swap(p, 1) for p in pieces]


def spread_half(mine, other):
    across = swap(other, 2)
    pieces = [mine, across, swap(mine, 4), swap(other, 6)]
    return pieces + [swap(p, 1) for p in pieces]


def give_back(chunks):
    blocks = lax.axis_size("blk")
    groups = lax.axis_size("uly")
    out = [chunks[0]]
    for n, c in enumerate(chunks[1:], 1):
        flip = n // groups * 2 * groups + n % groups
        pairs = [(i, i ^ flip) for i in range(blocks * groups)]
        out.append(lax.ppermute(c, ("blk", "uly"), pairs))
    return out


def cube_body(self_query, self_key, self_value, cross_query, text_key, text_value, padded_count):
    blocks = lax.axis_size("blk")
    groups = lax.axis_size("uly")
    block = lax.axis_index("blk")
    lane = lax.axis_index("uly")
    rows, channels = self_query.shape
    width = channels // groups
    shard_rows = rows * groups
    grid_width = TW * groups
    scaling = 1.0 / math.sqrt(HD)
    where = jnp.stack([lane, block, block // 2 % 2]).astype(jnp.int32)
    valid = blocks * shard_rows - padded_count[0]

    side = HD // 6
    first = HD // 2 - 2 * side
    pair = np.arange(HD) // 2
    bands = [pair < first, pair < first + side]
    step = np.select(bands, [pair / first, (pair - first) / side], (pair - first - side) / side)
    omega = jnp.asarray(10000.0**-step, jnp.float32)[None, :]

    shape = lambda n, w=width: jax.ShapeDtypeStruct((n, w), jnp.bfloat16)

    def pack_values(s, a, o):
        copy_chunks(s[0], a[0], o, 0)

    def pack_keys(s, a, o):
        rotate_chunks(s[0], s[1], a[0], a[1], o, 0)

    def stack_text(s, a, o):
        n = a[0].shape[0]
        o[0][:n, :] = a[0][...]
        o[0][n:, :] = a[1][...]

    def merge_chunks(s, a, o):
        for t, out in enumerate(o):
            cols = pl.ds(pl.multiple_of((s[2] ^ t) * out.shape[1], out.shape[1]), out.shape[1])
            for k, chunk in enumerate(a):
                out[pl.ds(pl.multiple_of((s[0] ^ k) * rows, rows), rows), :] = chunk[:, cols]

    def place_other(s, a, o):
        place_rows(a[0], a[1:], (1 - s[2]) * o[0].shape[1], o[0])

    def unpack_chunks(s, a, o):
        wide = a[0].shape[1]
        per = width // wide
        for n, chunk in enumerate(a):
            start = (s[0] ^ n % groups) * per + (s[2] ^ n // groups if per > 1 else 0)
            o[0][:, pl.ds(pl.multiple_of(start * wide, wide), wide)] = chunk[...]

    def merge(chunks):
        return call(merge_chunks, [shape(shard_rows, width // 2)] * 2, chunks, where)

    def unpack(chunks):
        return call(unpack_chunks, [shape(rows, channels)], chunks, where)[0]

    value_chunks = scatter(call(pack_values, [shape(rows)] * groups, [self_value], where))
    stacked = call(stack_text, [shape(2 * text_key.shape[0])], [text_key, text_value], where)[0]
    text = spread(stacked)
    packed = call(pack_keys, [shape(rows)] * groups, [omega, self_key], where)
    key_chunks = scatter(packed)
    values = spread_half(*merge(value_chunks))
    cross_chunks = scatter(call(pack_values, [shape(rows)] * groups, [cross_query], where))
    packed = call(pack_keys, [shape(rows)] * groups, [omega, self_query], where)
    query_chunks = scatter(packed)
    keys = spread_half(*merge(key_chunks))

    n = np.arange(shard_rows)
    offset = n % rows // TW * grid_width + n // rows * TW + n % TW
    r = lax.iota(jnp.int32, shard_rows)
    source = (lane ^ (r % rows // TW)) * rows + (lane ^ (r // rows)) * TW + r % TW
    place = (source[:, None] == r[None, :]).astype(jnp.bfloat16)
    half = shape(shard_rows, width // 2)
    other = call(place_other, [half], [place] + query_chunks, where)[0]
    across = swap(other, 2)
    flips = np.asarray([0, 2, 4, 6, 1, 3, 5, 7])
    owner = np.repeat(flips, shard_rows)
    inside = np.tile(offset, len(flips))
    position = (block ^ jnp.asarray(owner, jnp.int32)) * shard_rows + jnp.asarray(inside, jnp.int32)
    bias = jnp.where(position < valid, 0.0, neg_fill).astype(jnp.float32)[None, :]

    cross = attend(where, place, cross_chunks, bias, text, [], groups, width, True, scaling)
    cross_back = scatter(cross)
    wide = width // 2
    near = attend(where, place, query_chunks, bias, keys, values, groups, wide, False, scaling)
    far = attend(where, None, [across], bias, keys, values, groups, wide, False, scaling)
    self_back = give_back(near + far)
    return unpack(self_back), unpack(cross_back)


def body(*args):
    rows = args[0].shape[0]
    fits = lax.axis_size("blk") * lax.axis_size("uly") * rows <= 2048
    even = args[0].shape[1] // lax.axis_size("uly") // HD % 2 == 0
    if lax.axis_size("blk") == 8 and lax.axis_size("uly") == TH and fits and even:
        return cube_body(*args)
    return plain_body(*args)


def solution(mesh):
    in_specs = (
        P(("blk", "uly"), None),
        P(("blk", "uly"), None),
        P(("blk", "uly"), None),
        P(("blk", "uly"), None),
        P("blk", "uly"),
        P("blk", "uly"),
        P(),
    )
    out_specs = (P(("blk", "uly"), None), P(("blk", "uly"), None))
    return jax.shard_map(body, mesh=mesh, in_specs=in_specs, out_specs=out_specs, check_vma=False)
```
